32 devices in a mesh: ta: 4 (over y, x), sa: 8 (over z, core).
Axes of the slice: x: 2, y: 2, z: 4, core: 2. Of those that a mesh axis runs over, the one named last changes fastest.
Arguments:
- eigvecs: float32 [2, 8, 64, 3, 4096], P(None, 'ta', None, None, 'sa'), may hold values from -0.0546875 to 0.0546875
- solutions: float32 [2, 8, 3, 8, 4, 3, 4096], P(None, 'ta', None, None, None, None, 'sa'), may hold values from -15 to 15
- source_times: int32 [3], replicated, may hold values from 0 to 7, as said below
- spin_dilution: int32 [3, 8], replicated, may hold values from 0 to 3
Outputs:
- perambulator: float32 [2, 8, 6144], P(None, 'ta', 'sa')
- norms: float32 [3, 8], replicated
The draws below stay inside these ranges and needn't reach their ends.
Inputs may be any that keep to these rules, and one draw needn't show every extreme that they name: `source_times`: some source lies at slice 0 and another at slice 8 - 1.
All inputs are finite; a program needn't handle non-finite values.
Results may differ from the reference program's by a relative error of at most 0.000084.
Values sent between devices are 32-bit elements; how exact they have to be, the bound alone decides.
No kernel may reach another device: no remote copies, remote signals or barrier semaphores. Data moves between devices by JAX's collectives and lax.ppermute only.
A program may use at most 64 MiB of HBM per device.

```python
import jax
import jax.numpy as jnp
from jax import lax

NEV = 64
NSRC = 3
COLS = 8
NT = 8
NSPACE = 4096


def times_for(key):
    base = jax.random.randint(jax.random.fold_in(key, 7), (NSRC,), 0, NT).astype(jnp.int32)
    last_pick = jax.random.randint(jax.random.fold_in(key, 8), (), 0, NSRC).astype(jnp.int32)
    step_pick = jax.random.randint(jax.random.fold_in(key, 9), (), 1, NSRC).astype(jnp.int32)
    first_pick = (last_pick + step_pick) % NSRC
    slots = jnp.arange(NSRC, dtype=jnp.int32)
    base = jnp.where(slots == last_pick, NT - 1, base)
    base = jnp.where(slots == first_pick, 0, base)
    return base.astype(jnp.int32)


def draw_source_times(key, part):
    return times_for(key)


def solution_part(key, salt):
    starts = times_for(key)
    slice_ids = jnp.arange(NT, dtype=jnp.int32)
    apart = jnp.abs(slice_ids[:, None] - starts[None, :])
    apart = jnp.minimum(apart, NT - apart).astype(jnp.float32)
    amplitude = 0.5 + 2.5 * jnp.exp(-apart * 16.0 / NT)
    shape = (NT, NSRC, COLS, 4, 3, NSPACE)
    noise_key = jax.random.fold_in(key, salt)
    noise = jnp.clip(jax.random.normal(noise_key, shape, jnp.float32), -5.0, 5.0)
    return noise * amplitude[:, :, None, None, None, None]


def draw_solutions(key, part):
    return jnp.stack([solution_part(key, 11), solution_part(key, 13)]).astype(jnp.float32)


def plant(entries, key, least, high):
    longest = entries.shape.index(max(entries.shape))
    spots = []
    for shift in (0, 1):
        where = [jax.random.randint(jax.random.fold_in(key, axis), (), 0, length) for axis, length in enumerate(entries.shape)]
        where[longest] = (where[longest] + shift) % entries.shape[longest]
        spots.append(tuple(where))
    return entries.at[spots[0]].set(least).at[spots[1]].set(high)


def level_of(stream_key, extent, shards, smallest, top_value):
    level = 1.0
    for dim, shards_of in shards:
        steps = jax.random.uniform(jax.random.fold_in(jax.random.fold_in(stream_key, 6), dim), (shards_of,), jnp.float32, smallest / len(shards), top_value / len(shards))
        level = level * jnp.repeat(jnp.exp(steps), extent[dim] // shards_of).reshape((-1,) + (1,) * (len(extent) - 1 - dim))
    return level


def centred(own_key, shape, width, bound, pieces=(), held_as=jnp.bfloat16):
    loudness = level_of(own_key, shape, pieces, -0.22, 0.18) if pieces else 1.0
    array = jax.random.normal(own_key, shape, jnp.float32) * width * loudness
    return jnp.minimum(jnp.maximum(array, -bound), bound).astype(held_as)


def setup_inputs(seed: int = 0) -> dict:
    seeds = jax.random.split(jax.random.key(seed), 5)
    eigvecs = centred(seeds[0], (2, NT, NEV, 3, NSPACE), (3 * NSPACE) ** -0.5, 0.0546875, ((1, 4), (4, 8)), jnp.float32)
    solutions = draw_solutions(jax.random.fold_in(seeds[4], 71), 0)
    source_times = draw_source_times(jax.random.fold_in(seeds[4], 71), 0)
    spin_dilution = plant(jax.random.randint(seeds[3], (NSRC, COLS), 0, 4), jax.random.fold_in(seeds[3], 1), 0, 3).astype(jnp.int32)
    return dict(eigvecs=eigvecs, solutions=solutions, source_times=source_times, spin_dilution=spin_dilution)


def slice_tile(inputs):
    eig_real, eig_imag, sol_real, sol_imag = inputs
    precise = lax.Precision.HIGHEST
    real_part = jnp.dot(eig_real, sol_real.T, precision=precise, preferred_element_type=jnp.float32) + jnp.dot(eig_imag, sol_imag.T, precision=precise, preferred_element_type=jnp.float32)
    imag_part = jnp.dot(eig_real, sol_imag.T, precision=precise, preferred_element_type=jnp.float32) - jnp.dot(eig_imag, sol_real.T, precision=precise, preferred_element_type=jnp.float32)
    return jnp.stack([real_part, imag_part])


def reference(eigvecs, solutions, source_times, spin_dilution):
    slice_count = eigvecs.shape[1]
    eig_count = eigvecs.shape[2]
    site_count = eigvecs.shape[4]
    src_count = spin_dilution.shape[0]
    col_count = spin_dilution.shape[1]
    columns = src_count * col_count * 4
    inner_len = 3 * site_count
    eigen_rows = eigvecs.reshape(2, slice_count, eig_count, inner_len)
    solution_rows = solutions.reshape(2, slice_count, columns, inner_len)
    tiles = lax.map(slice_tile, (eigen_rows[0], eigen_rows[1], solution_rows[0], solution_rows[1]))
    tiles = jnp.transpose(tiles, (1, 0, 2, 3))
    slice_times = jnp.arange(slice_count, dtype=jnp.int32)
    boundary = jnp.where(slice_times[:, None] < source_times[None, :], -1.0, 1.0).astype(jnp.float32)
    chirality = jnp.where(spin_dilution < 2, 1.0, -1.0).astype(jnp.float32)
    signs = jnp.broadcast_to((boundary[:, :, None] * chirality[None])[:, :, :, None], (slice_count, src_count, col_count, 4)).reshape(slice_count, columns)
    perambulator = (tiles * signs[None, :, None, :]).reshape(2, slice_count, eig_count * columns)
    norms = jnp.sum(solutions * solutions, axis=(0, 1, 4, 5, 6)) / (12.0 * slice_count * site_count)
    return perambulator, norms
```

```python
import functools

import jax
import jax.numpy as jnp
from jax import lax
from jax.experimental import pallas as pl
from jax.experimental.pallas import tpu as pltpu
from jax.sharding import PartitionSpec as P

F32 = jnp.float32
BF16 = jnp.bfloat16
SPINS = 4
COLORS = 3
LANES = 128
NT_DIMS = (((1,), (1,)), ((), ()))


def halves(x):
    high = x.astype(BF16)
    return high, (x - high.astype(F32)).astype(BF16)


def dot_nt(a, b, precision=None):
    return lax.dot_general(a, b, NT_DIMS, precision=precision, preferred_element_type=F32)


def project_kernel(e_hbm, s_hbm, o_ref, e_v, s_v, e_sem, s_sem, *, pairs):
    rows_t = e_hbm.shape[1]
    eigs = e_hbm.shape[3]
    sites = e_hbm.shape[4]
    blocks = sites // LANES
    columns = pairs * SPINS
    copies = {}
    for t in range(rows_t):
        for part in range(2):
            s_copy = pltpu.make_async_copy(s_hbm.at[part, t], s_v.at[part, t], s_sem.at[part, t])
            e_copy = pltpu.make_async_copy(e_hbm.at[part, t], e_v.at[part, t], e_sem.at[part, t])
            s_copy.start()
            e_copy.start()
            copies[part, t] = (s_copy, e_copy)
    squares = jnp.zeros((pairs, LANES), F32)
    for t in range(rows_t):
        for part in range(2):
            for copy in copies[part, t]:
                copy.wait()
        total = jnp.zeros((2 * eigs, 2 * LANES), F32)
        for color in range(COLORS):
            stack = []
            for part in range(2):
                wide = []
                for block in range(blocks):
                    first = (color * blocks + block) * SPINS
                    step = COLORS * blocks * SPINS
                    spins = [
                        s_v[part, t, pl.ds(first + spin, pairs, stride=step), :]
                        for spin in range(SPINS)
                    ]
                    for rows in spins:
                        squares = squares + rows * rows
                    wide.append(jnp.concatenate(spins, 0))
                stack.append(jnp.concatenate(wide, 1))
                stack.append(jnp.zeros((LANES - columns, sites), F32))
            s_high, s_low = halves(jnp.concatenate(stack, 0))
            e_high, e_low = halves(jnp.concatenate([e_v[0, t, color], e_v[1, t, color]], 0))
            total = total + dot_nt(e_high, s_high)
            total = total + dot_nt(e_low, s_high)
            total = total + dot_nt(e_high, s_low)
        o_ref[:, t] = (total[:eigs, :LANES] + total[eigs:, LANES:]).reshape(-1, 8, LANES)
        o_ref[:, rows_t + t] = (total[:eigs, LANES:] - total[eigs:, :LANES]).reshape(-1, 8, LANES)
    placed = jnp.concatenate(
        [
            jnp.zeros((columns, LANES), F32),
            squares,
            jnp.zeros((LANES - columns - pairs, LANES), F32),
        ],
        0,
    )
    norm_row = dot_nt(jnp.ones((8, LANES), F32), placed, lax.Precision.HIGHEST)
    for group in range(eigs // 8):
        o_ref[group, 0] = o_ref[group, 0] + norm_row


def project(eigvecs, solutions):
    _, rows_t, eigs, _, sites = eigvecs.shape
    pairs = solutions.shape[2] * solutions.shape[3]
    blocks = sites // LANES
    e_view = jnp.transpose(eigvecs, (0, 1, 3, 2, 4))
    s_view = jnp.transpose(solutions, (0, 1, 2, 3, 5, 4, 6))
    s_view = s_view.reshape(2, rows_t, pairs, COLORS, SPINS, blocks, LANES)
    s_view = jnp.swapaxes(s_view, 4, 5).reshape(2, rows_t, -1, LANES)
    e_view = pltpu.with_memory_space_constraint(e_view, pltpu.HBM)
    s_view = pltpu.with_memory_space_constraint(s_view, pltpu.HBM)
    return pl.pallas_call(
        functools.partial(project_kernel, pairs=pairs),
        out_shape=jax.ShapeDtypeStruct((eigs // 8, 2 * rows_t, 8, LANES), F32),
        in_specs=[pl.BlockSpec(memory_space=pltpu.HBM)] * 2,
        out_specs=pl.BlockSpec(memory_space=pltpu.VMEM),
        scratch_shapes=[
            pltpu.VMEM(e_view.shape, F32),
            pltpu.VMEM(s_view.shape, F32),
            pltpu.SemaphoreType.DMA((2, rows_t)),
            pltpu.SemaphoreType.DMA((2, rows_t)),
        ],
        compiler_params=pltpu.CompilerParams(vmem_limit_bytes=40 * 2**20),
        cost_estimate=pl.CostEstimate(
            flops=2 * 3 * 4 * rows_t * eigs * pairs * SPINS * COLORS * sites,
            bytes_accessed=4 * (eigvecs.size + solutions.size),
            transcendentals=0,
        ),
    )(e_view, s_view)


def radices_of(count):
    found = []
    for prime in (2, 3, 5, 7, 11, 13):
        while count % prime == 0:
            found.append(prime)
            count //= prime
    return found + ([count] if count > 1 else [])


def scatter_sum(blocks, axis):
    size = lax.axis_size(axis)
    me = lax.axis_index(axis)
    radices = radices_of(size)
    shape = blocks.shape[1:]
    held = blocks.reshape(tuple(reversed(radices)) + shape)
    weight = 1
    for depth, radix in enumerate(radices):
        axis_no = len(radices) - 1 - depth
        digit = (me // weight) % radix
        total = lax.dynamic_index_in_dim(held, digit, axis_no, False)
        for shift in range(1, radix):
            send = lax.dynamic_index_in_dim(held, (digit + shift) % radix, axis_no, False)
            pairs = []
            for source in range(size):
                own = (source // weight) % radix
                pairs.append((source, source + ((own + shift) % radix - own) * weight))
            total = total + lax.ppermute(send, axis, pairs)
        held = total
        weight *= radix
    return held


def all_sum(x, axis):
    size = lax.axis_size(axis)
    weight = 1
    for radix in radices_of(size):
        total = x
        for shift in range(1, radix):
            pairs = []
            for source in range(size):
                own = (source // weight) % radix
                pairs.append((source, source + ((own + shift) % radix - own) * weight))
            total = total + lax.ppermute(x, axis, pairs)
        x = total
        weight *= radix
    return x


def on_device(eigvecs, solutions, source_times, spin_dilution):
    _, rows_t, eigs, _, sites = eigvecs.shape
    src_count, col_count = spin_dilution.shape
    pairs = src_count * col_count
    columns = pairs * SPINS
    devices = lax.axis_size("sa")
    all_cells = 12.0 * rows_t * lax.axis_size("ta") * sites * devices
    own_width = eigs * columns // devices

    tiles = project(eigvecs, solutions)
    slice_times = lax.axis_index("ta") * rows_t + jnp.arange(rows_t, dtype=jnp.int32)
    boundary = jnp.where(slice_times[:, None] < source_times[None, :], -1.0, 1.0).astype(F32)
    chirality = jnp.where(spin_dilution < 2, 1.0, -1.0).astype(F32)
    signs = (boundary[:, :, None] * chirality[None]).reshape(rows_t, pairs)
    if eigs % devices == 0 and (eigs // devices) % 8 == 0:
        groups = eigs // devices // 8
        mine = scatter_sum(tiles.reshape(devices, groups, 2 * rows_t, 8, LANES), "sa")
        norm_row = mine[0, 0, 0, columns : columns + pairs]
        values = mine.reshape(groups, 2, rows_t, 8, LANES)[..., :columns]
        values = values.reshape(groups, 2, rows_t, 8, SPINS, pairs) * signs[None, None, :, None, None]
        values = jnp.transpose(values, (1, 2, 0, 3, 5, 4)).reshape(2, rows_t, own_width)
    else:
        norm_row = lax.psum(tiles[0, 0, 0, columns : columns + pairs], "sa")
        values = tiles.reshape(eigs // 8, 2, rows_t, 8, LANES)[..., :columns]
        values = values.reshape(eigs // 8, 2, rows_t, 8, SPINS, pairs) * signs[None, None, :, None, None]
        values = jnp.transpose(values, (1, 2, 0, 3, 5, 4)).reshape(2, rows_t, devices, own_width)
        values = scatter_sum(jnp.transpose(values, (2, 0, 1, 3)), "sa")
    norms = all_sum(norm_row.reshape(src_count, col_count), "ta") / all_cells
    return values, norms


def solution(mesh):
    return jax.shard_map(
        on_device,
        mesh=mesh,
        in_specs=(
            P(None, "ta", None, None, "sa"),
            P(None, "ta", None, None, None, None, "sa"),
            P(),
            P(),
        ),
        out_specs=(P(None, "ta", "sa"), P()),
        check_vma=False,
    )
```

```python
import functools

import jax
import jax.numpy as jnp
from jax import lax
from jax.experimental import pallas as pl
from jax.experimental.pallas import tpu as pltpu
from jax.sharding import PartitionSpec as P

F32 = jnp.float32
BF16 = jnp.bfloat16
SPINS = 4
COLORS = 3
LANES = 128
NT_DIMS = (((1,), (1,)), ((), ()))
VMEM_BYTES = 32 * 2**20


def halves(x):
    high = x.astype(BF16)
    return high, (x - high.astype(F32)).astype(BF16)


def dot_nt(a, b, precision=None):
    return lax.dot_general(a, b, NT_DIMS, precision=precision, preferred_element_type=F32)


def split_kernel(s_hbm, split_ref, norm_ref, s_v, sems):
    _, times, pairs, rows, _ = s_hbm.shape
    columns = SPINS * pairs
    blocks = rows // (COLORS * SPINS)
    pitch = s_v.shape[3]
    copies = {}
    for t in range(times):
        for part in range(2):
            copy = pltpu.make_async_copy(
                s_hbm.at[part, t], s_v.at[part, t, :, pl.ds(0, rows)], sems.at[part, t]
            )
            copy.start()
            copies[part, t] = copy
    squares = [jnp.zeros((pairs, LANES), F32) for _ in range(2)]
    for t in range(times):
        for part in range(2):
            copies[part, t].wait()
            flat = s_v.at[part, t].reshape(pairs * pitch, LANES)
            for block in range(COLORS * blocks):
                spins = [
                    flat[pl.ds(block * SPINS + spin, pairs, stride=pitch), :]
                    for spin in range(SPINS)
                ]
                for spin in range(SPINS):
                    squares[spin % 2] = squares[spin % 2] + spins[spin] * spins[spin]
                high, low = halves(jnp.concatenate(spins, 0))
                lanes = slice(block * LANES, (block + 1) * LANES)
                split_ref[t, part * columns : (part + 1) * columns, lanes] = high
                split_ref[t, (2 + part) * columns : (3 + part) * columns, lanes] = low
    placed = jnp.concatenate(
        [
            jnp.zeros((columns, LANES), F32),
            squares[0] + squares[1],
            jnp.zeros((LANES - columns - pairs, LANES), F32),
        ],
        0,
    )
    norm_ref[...] = dot_nt(jnp.ones((8, LANES), F32), placed, lax.Precision.HIGHEST)


def tile_kernel(split_ref, e_ref, norm_ref, *refs, roles):
    _, times, _, eigs, sites = e_ref.shape
    columns = split_ref.shape[1] // 4
    tiles = refs[-1]
    lane = lax.broadcasted_iota(jnp.int32, (columns, LANES), 1)
    for t in range(times):
        wide = []
        for color in range(COLORS):
            stack = jnp.concatenate([e_ref[0, t, color], e_ref[1, t, color]], 0)
            wide.append(jnp.concatenate(halves(stack), 0))
        product = dot_nt(split_ref[t], jnp.concatenate(wide, 1))
        top = product[: 2 * columns]
        joint = top[:, : 2 * eigs] + top[:, 2 * eigs :] + product[2 * columns :, : 2 * eigs]
        real = joint[:columns]
        imag = pltpu.roll(joint[columns:], eigs, 1)
        both = imag + jnp.where(lane < eigs, real, -real)
        both = jnp.concatenate([both, jnp.zeros((LANES - columns, LANES), F32)], 0).T
        both = both.reshape(2, eigs // 8, 8, LANES)
        tiles[:, t] = both[0] + norm_ref[...] if t == 0 else both[0]
        tiles[:, times + t] = both[1]
    if roles:
        near_ref, far_ref = refs[:2]
        chip = lax.axis_index("sa") // 2
        for pos in range(2):
            for core in range(2):
                near_ref[pos, core] = tiles[2 * jnp.bitwise_xor(chip, 2 * pos) + core]
                far_ref[pos, core] = tiles[2 * jnp.bitwise_xor(chip, 2 * pos + 1) + core]


def local_tiles(eigvecs, solutions, roles):
    _, times, eigs, _, sites = eigvecs.shape
    pairs = solutions.shape[2] * solutions.shape[3]
    columns = pairs * SPINS
    blocks = sites // LANES
    rows = COLORS * blocks * SPINS
    pitch = rows + 8 if (rows // 8) % 2 == 0 else rows
    e_view = jnp.transpose(eigvecs, (0, 1, 3, 2, 4))
    s_view = jnp.transpose(solutions, (0, 1, 2, 3, 5, 4, 6))
    s_view = s_view.reshape(2, times, pairs, COLORS, SPINS, blocks, LANES)
    s_view = jnp.swapaxes(s_view, 4, 5).reshape(2, times, pairs, rows, LANES)
    s_view = pltpu.with_memory_space_constraint(s_view, pltpu.HBM)
    vmem = pl.BlockSpec(memory_space=pltpu.VMEM)
    params = pltpu.CompilerParams(vmem_limit_bytes=VMEM_BYTES)
    split, norm_row = pl.pallas_call(
        split_kernel,
        out_shape=(
            jax.ShapeDtypeStruct((times, 4 * columns, COLORS * sites), BF16),
            jax.ShapeDtypeStruct((8, LANES), F32),
        ),
        in_specs=[pl.BlockSpec(memory_space=pltpu.HBM)],
        out_specs=(vmem, vmem),
        scratch_shapes=[
            pltpu.VMEM((2, times, pairs, pitch, LANES), F32),
            pltpu.SemaphoreType.DMA((2, times)),
        ],
        compiler_params=params,
        name="split",
        cost_estimate=pl.CostEstimate(
            flops=8 * solutions.size, bytes_accessed=8 * solutions.size, transcendentals=0
        ),
    )(s_view)
    tiles = jax.ShapeDtypeStruct((eigs // 8, 2 * times, 8, LANES), F32)
    block = jax.ShapeDtypeStruct((2, 2, 2 * times, 8, LANES), F32)
    return pl.pallas_call(
        functools.partial(tile_kernel, roles=roles),
        out_shape=(block, block) if roles else tiles,
        in_specs=[vmem] * 3,
        out_specs=(vmem, vmem) if roles else vmem,
        scratch_shapes=[pltpu.VMEM(tiles.shape, F32)] if roles else [],
        compiler_params=params,
        name="tiles",
        cost_estimate=pl.CostEstimate(
            flops=24 * times * eigs * columns * COLORS * sites,
            bytes_accessed=4 * (eigvecs.size + solutions.size),
            transcendentals=0,
        ),
    )(split, e_view, norm_row)


def finish_kernel(near_ref, mine_ref, south_ref, north_ref, extra_ref, sign_ref, out_ref, norm_ref, *, cells):
    _, times, width = out_ref.shape
    src_count, col_count = norm_ref.shape
    columns = width // 8
    pairs = columns // SPINS
    north = (lax.axis_index("sa") % 2) == 1
    row = lax.broadcasted_iota(jnp.int32, (8, LANES), 0)
    lane = lax.broadcasted_iota(jnp.int32, (8, LANES), 1)
    column = jnp.bitwise_and(lane + LANES - (row * columns) % LANES, LANES - 1)
    source = jnp.where(column < columns, (column % SPINS) * pairs + column // SPINS, 0)
    for part in range(2):
        for t in range(times):
            index = part * times + t
            as_north = mine_ref[index] + north_ref[1, index]
            if index == 0:
                as_north = as_north + extra_ref[...]
            tile = jnp.where(north, as_north, near_ref[0, 0, index] + south_ref[index])
            if index == 0:
                for src in range(src_count):
                    shift = 2 * LANES - columns - src * col_count
                    norm_ref[src : src + 1, :] = (
                        pltpu.roll(tile, shift % LANES, 1)[:1, :col_count] / cells
                    )
            tile = tile * sign_ref[t : t + 1, :]
            tile = jnp.take_along_axis(tile, source, axis=1)
            for piece in range(width // LANES):
                first = piece * LANES // columns
                edge = (first + 1) * columns - piece * LANES
                out_ref[part, t : t + 1, piece * LANES : (piece + 1) * LANES] = jnp.where(
                    lane[:1] < edge, tile[first : first + 1], tile[min(first + 1, 7) : min(first + 1, 7) + 1]
                )


def one_way(x, moves):
    ta_size, sa_size = lax.axis_size("ta"), lax.axis_size("sa")
    pairs = []
    for ta in range(ta_size):
        for sa in range(sa_size):
            to = moves(ta, sa // 2, sa % 2)
            if to is not None:
                pairs.append((ta * sa_size + sa, to[0] * sa_size + to[1] * 2 + to[2]))
    return lax.ppermute(x, ("ta", "sa"), pairs)


def exchange_by_roles(near, far):
    tail = lax.broadcasted_iota(jnp.int32, (8, LANES), 1) >= LANES - 32
    first = (lax.broadcasted_iota(jnp.int32, (near.shape[2], 1, 1), 0) == 0)

    def with_tail(blocks, extra):
        return blocks + jnp.where(first, extra, 0.0)

    far = far + one_way(far, lambda ta, z, c: (ta, z, 1) if c == 0 else None)
    near_in = one_way(near, lambda ta, z, c: (ta, z, 0) if c == 1 else None)
    side = far[0, 0, 0]
    z1 = one_way(far, lambda ta, z, c: (ta, z ^ 1, 0) if c == 1 else None)
    x0 = one_way(side, lambda ta, z, c: (ta ^ 1, z, 0) if c == 1 else None)
    x1 = one_way(side, lambda ta, z, c: (ta ^ 1, z ^ 1, 0) if c == 1 else None)
    near = with_tail(near + near_in + z1, jnp.where(tail, x0 + x1, 0.0))
    side = near[0, 0, 0]
    z2 = one_way(near[1], lambda ta, z, c: (ta, z ^ 2, 1) if c == 0 else None)
    y0 = one_way(side, lambda ta, z, c: (ta ^ 2, z, 1) if c == 0 else None)
    y1 = one_way(side, lambda ta, z, c: (ta ^ 2, z ^ 2, 1) if c == 0 else None)
    mine = one_way(near[0, 1], lambda ta, z, c: (ta, z, 1) if c == 0 else None)
    extra = jnp.where(tail, y0 + y1, 0.0)
    south = one_way(with_tail(z2[0], extra), lambda ta, z, c: (ta, z, 0) if c == 1 else None)
    return near, mine, south, z2, extra


def radices_of(count):
    found = []
    for prime in (2, 3, 5, 7, 11, 13):
        while count % prime == 0:
            found.append(prime)
            count //= prime
    return found + ([count] if count > 1 else [])


def shifted(size, weight, radix, shift):
    moves = []
    for source in range(size):
        own = (source // weight) % radix
        moves.append((source, source + ((own + shift) % radix - own) * weight))
    return moves


def scatter_sum(blocks, axis):
    size = lax.axis_size(axis)
    me = lax.axis_index(axis)
    radices = radices_of(size)
    held = blocks.reshape(tuple(reversed(radices)) + blocks.shape[1:])
    weight = 1
    for depth, radix in enumerate(radices):
        dim = len(radices) - 1 - depth
        digit = (me // weight) % radix
        total = lax.dynamic_index_in_dim(held, digit, dim, False)
        for shift in range(1, radix):
            send = lax.dynamic_index_in_dim(held, (digit + shift) % radix, dim, False)
            total = total + lax.ppermute(send, axis, shifted(size, weight, radix, shift))
        held = total
        weight *= radix
    return held


def all_sum(x, axis):
    size = lax.axis_size(axis)
    weight = 1
    for radix in radices_of(size):
        total = x
        for shift in range(1, radix):
            total = total + lax.ppermute(x, axis, shifted(size, weight, radix, shift))
        x = total
        weight *= radix
    return x


def on_device(eigvecs, solutions, source_times, spin_dilution):
    _, times, eigs, _, sites = eigvecs.shape
    src_count, col_count = spin_dilution.shape
    pairs = src_count * col_count
    columns = pairs * SPINS
    devices = lax.axis_size("sa")
    cells = 12.0 * times * lax.axis_size("ta") * sites * devices
    own_width = eigs * columns // devices

    roles = devices == 8 and lax.axis_size("ta") == 4 and eigs == 64 and columns == 96
    tiles = local_tiles(eigvecs, solutions, roles)
    slice_times = lax.axis_index("ta") * times + jnp.arange(times, dtype=jnp.int32)
    boundary = jnp.where(slice_times[:, None] < source_times[None, :], -1.0, 1.0).astype(F32)
    chirality = jnp.where(spin_dilution < 2, 1.0, -1.0).astype(F32)
    signs = (boundary[:, :, None] * chirality[None]).reshape(times, pairs)
    if roles:
        near, mine, south, north, extra = exchange_by_roles(*tiles)
        lanes = jnp.concatenate(
            [signs] * SPINS + [jnp.ones((times, LANES - columns), F32)], 1
        )
        vmem = pl.BlockSpec(memory_space=pltpu.VMEM)
        return pl.pallas_call(
            functools.partial(finish_kernel, cells=cells),
            out_shape=(
                jax.ShapeDtypeStruct((2, times, own_width), F32),
                jax.ShapeDtypeStruct((src_count, col_count), F32),
            ),
            in_specs=[vmem] * 6,
            out_specs=(vmem, vmem),
            compiler_params=pltpu.CompilerParams(vmem_limit_bytes=VMEM_BYTES),
            name="finish",
        )(near, mine, south, north, extra, lanes)
    norm_row = lax.psum(tiles[0, 0, 0, columns : columns + pairs], "sa")
    values = tiles.reshape(eigs // 8, 2, times, 8, LANES)[..., :columns]
    values = values.reshape(eigs // 8, 2, times, 8, SPINS, pairs)
    values = values * signs[None, None, :, None, None]
    values = jnp.transpose(values, (1, 2, 0, 3, 5, 4)).reshape(2, times, devices, own_width)
    values = scatter_sum(jnp.transpose(values, (2, 0, 1, 3)), "sa")
    norms = all_sum(norm_row.reshape(src_count, col_count), "ta") / cells
    return values, norms


def solution(mesh):
    return jax.shard_map(
        on_device,
        mesh=mesh,
        in_specs=(
            P(None, "ta", None, None, "sa"),
            P(None, "ta", None, None, None, None, "sa"),
            P(),
            P(),
        ),
        out_specs=(P(None, "ta", "sa"), P()),
        check_vma=False,
    )
```

```python
import functools

import jax
import jax.numpy as jnp
from jax import lax
from jax.experimental import pallas as pl
from jax.experimental.pallas import tpu as pltpu
from jax.sharding import PartitionSpec as P

F32 = jnp.float32
BF16 = jnp.bfloat16
SPINS = 4
COLORS = 3
LANES = 128
NT_DIMS = (((1,), (1,)), ((), ()))
VMEM_BYTES = 32 * 2**20
MASKS = (1, 3, 5)


def halves(x):
    high = x.astype(BF16)
    return high, (x - high.astype(F32)).astype(BF16)


def dot_nt(a, b, precision=None):
    return lax.dot_general(a, b, NT_DIMS, precision=precision, preferred_element_type=F32)


def split_kernel(s_hbm, split_ref, norm_ref, s_v, sems):
    _, times, pairs, rows, _ = s_hbm.shape
    columns = SPINS * pairs
    blocks = rows // (COLORS * SPINS)
    pitch = s_v.shape[3]
    copies = {}
    for t in range(times):
        for part in range(2):
            copy = pltpu.make_async_copy(
                s_hbm.at[part, t], s_v.at[part, t, :, pl.ds(0, rows)], sems.at[part, t]
            )
            copy.start()
            copies[part, t] = copy
    squares = [jnp.zeros((pairs, LANES), F32) for _ in range(2)]
    for t in range(times):
        for part in range(2):
            copies[part, t].wait()
            flat = s_v.at[part, t].reshape(pairs * pitch, LANES)
            for block in range(COLORS * blocks):
                spins = [
                    flat[pl.ds(block * SPINS + spin, pairs, stride=pitch), :]
                    for spin in range(SPINS)
                ]
                for spin in range(SPINS):
                    squares[spin % 2] = squares[spin % 2] + spins[spin] * spins[spin]
                high, low = halves(jnp.concatenate(spins, 0))
                lanes = slice(block * LANES, (block + 1) * LANES)
                split_ref[t, part * columns : (part + 1) * columns, lanes] = high
                split_ref[t, (2 + part) * columns : (3 + part) * columns, lanes] = low
    placed = jnp.concatenate(
        [
            jnp.zeros((columns, LANES), F32),
            squares[0] + squares[1],
            jnp.zeros((LANES - columns - pairs, LANES), F32),
        ],
        0,
    )
    norm_ref[...] = dot_nt(jnp.ones((8, LANES), F32), placed, lax.Precision.HIGHEST)


def tile_kernel(split_ref, e_ref, *refs, masks):
    _, times, _, eigs, _ = e_ref.shape
    columns = split_ref.shape[1] // 4
    tiles = refs[-1]
    lane = lax.broadcasted_iota(jnp.int32, (columns, LANES), 1)
    for t in range(times):
        wide = []
        for color in range(COLORS):
            stack = jnp.concatenate([e_ref[0, t, color], e_ref[1, t, color]], 0)
            wide.append(jnp.concatenate(halves(stack), 0))
        product = dot_nt(split_ref[t], jnp.concatenate(wide, 1))
        top = product[: 2 * columns]
        joint = top[:, : 2 * eigs] + top[:, 2 * eigs :] + product[2 * columns :, : 2 * eigs]
        real = joint[:columns]
        imag = pltpu.roll(joint[columns:], eigs, 1)
        both = imag + jnp.where(lane < eigs, real, -real)
        both = jnp.concatenate([both, jnp.zeros((LANES - columns, LANES), F32)], 0).T
        both = both.reshape(2, eigs // 8, 8, LANES)
        tiles[:, t] = both[0]
        tiles[:, times + t] = both[1]
    if masks:
        me = lax.axis_index("sa")
        for number, out_ref in enumerate(refs[:2]):
            for high in range(2):
                for low in range(2):
                    mask = number * masks[0] ^ high * masks[1] ^ low * masks[2]
                    out_ref[high, low] = tiles[jnp.bitwise_xor(me, mask)]


def local_tiles(eigvecs, solutions, masks):
    _, times, eigs, _, sites = eigvecs.shape
    pairs = solutions.shape[2] * solutions.shape[3]
    columns = pairs * SPINS
    blocks = sites // LANES
    rows = COLORS * blocks * SPINS
    pitch = rows + 8 if (rows // 8) % 2 == 0 else rows
    e_view = jnp.transpose(eigvecs, (0, 1, 3, 2, 4))
    s_view = jnp.transpose(solutions, (0, 1, 2, 3, 5, 4, 6))
    s_view = s_view.reshape(2, times, pairs, COLORS, SPINS, blocks, LANES)
    s_view = jnp.swapaxes(s_view, 4, 5).reshape(2, times, pairs, rows, LANES)
    s_view = pltpu.with_memory_space_constraint(s_view, pltpu.HBM)
    vmem = pl.BlockSpec(memory_space=pltpu.VMEM)
    params = pltpu.CompilerParams(vmem_limit_bytes=VMEM_BYTES)
    split, norm_row = pl.pallas_call(
        split_kernel,
        out_shape=(
            jax.ShapeDtypeStruct((times, 4 * columns, COLORS * sites), BF16),
            jax.ShapeDtypeStruct((8, LANES), F32),
        ),
        in_specs=[pl.BlockSpec(memory_space=pltpu.HBM)],
        out_specs=(vmem, vmem),
        scratch_shapes=[
            pltpu.VMEM((2, times, pairs, pitch, LANES), F32),
            pltpu.SemaphoreType.DMA((2, times)),
        ],
        compiler_params=params,
        name="split",
        cost_estimate=pl.CostEstimate(
            flops=8 * solutions.size, bytes_accessed=8 * solutions.size, transcendentals=0
        ),
    )(s_view)
    tiles = jax.ShapeDtypeStruct((eigs // 8, 2 * times, 8, LANES), F32)
    block = jax.ShapeDtypeStruct((2, 2, 2 * times, 8, LANES), F32)
    products = pl.pallas_call(
        functools.partial(tile_kernel, masks=masks),
        out_shape=(block, block) if masks else tiles,
        in_specs=[vmem] * 2,
        out_specs=(vmem, vmem) if masks else vmem,
        scratch_shapes=[pltpu.VMEM(tiles.shape, F32)] if masks else [],
        compiler_params=params,
        name="tiles",
        cost_estimate=pl.CostEstimate(
            flops=24 * times * eigs * columns * COLORS * sites,
            bytes_accessed=4 * (eigvecs.size + solutions.size),
            transcendentals=0,
        ),
    )(split, e_view)
    return products, norm_row


def finish_kernel(kept_ref, came_ref, extra_ref, sign_ref, out_ref, norm_ref, *, cells):
    _, times, width = out_ref.shape
    src_count, col_count = norm_ref.shape
    columns = width // 8
    pairs = columns // SPINS
    row = lax.broadcasted_iota(jnp.int32, (8, LANES), 0)
    lane = lax.broadcasted_iota(jnp.int32, (8, LANES), 1)
    column = jnp.bitwise_and(lane + LANES - (row * columns) % LANES, LANES - 1)
    source = jnp.where(column < columns, (column % SPINS) * pairs + column // SPINS, 0)
    for part in range(2):
        for t in range(times):
            index = part * times + t
            tile = kept_ref[index] + came_ref[index]
            if index == 0:
                for src in range(src_count):
                    shift = 2 * LANES - columns - src * col_count
                    norm = pltpu.roll(tile + extra_ref[...], shift % LANES, 1)
                    norm_ref[src : src + 1, :] = norm[:1, :col_count] / cells
            tile = tile * sign_ref[t : t + 1, :]
            tile = jnp.take_along_axis(tile, source, axis=1)
            for piece in range(width // LANES):
                first = piece * LANES // columns
                edge = (first + 1) * columns - piece * LANES
                out_ref[part, t : t + 1, piece * LANES : (piece + 1) * LANES] = jnp.where(
                    lane[:1] < edge, tile[first : first + 1], tile[first + 1 : first + 2]
                )


def swap(x, ta_mask, sa_mask):
    ta_size, sa_size = lax.axis_size("ta"), lax.axis_size("sa")
    pairs = [
        (ta * sa_size + sa, (ta ^ ta_mask) * sa_size + (sa ^ sa_mask))
        for ta in range(ta_size)
        for sa in range(sa_size)
    ]
    return lax.ppermute(x, ("ta", "sa"), pairs)


def radices_of(count):
    found = []
    for prime in (2, 3, 5, 7, 11, 13):
        while count % prime == 0:
            found.append(prime)
            count //= prime
    return found + ([count] if count > 1 else [])


def shifted(size, weight, radix, shift):
    moves = []
    for source in range(size):
        own = (source // weight) % radix
        moves.append((source, source + ((own + shift) % radix - own) * weight))
    return moves


def scatter_sum(blocks, axis):
    size = lax.axis_size(axis)
    me = lax.axis_index(axis)
    radices = radices_of(size)
    held = blocks.reshape(tuple(reversed(radices)) + blocks.shape[1:])
    weight = 1
    for depth, radix in enumerate(radices):
        dim = len(radices) - 1 - depth
        digit = (me // weight) % radix
        total = lax.dynamic_index_in_dim(held, digit, dim, False)
        for shift in range(1, radix):
            send = lax.dynamic_index_in_dim(held, (digit + shift) % radix, dim, False)
            total = total + lax.ppermute(send, axis, shifted(size, weight, radix, shift))
        held = total
        weight *= radix
    return held


def all_sum(x, axis):
    size = lax.axis_size(axis)
    weight = 1
    for radix in radices_of(size):
        total = x
        for shift in range(1, radix):
            total = total + lax.ppermute(x, axis, shifted(size, weight, radix, shift))
        x = total
        weight *= radix
    return x


def on_device(eigvecs, solutions, source_times, spin_dilution):
    _, times, eigs, _, sites = eigvecs.shape
    src_count, col_count = spin_dilution.shape
    pairs = src_count * col_count
    columns = pairs * SPINS
    devices = lax.axis_size("sa")
    cells = 12.0 * times * lax.axis_size("ta") * sites * devices
    own_width = eigs * columns // devices

    crossed = devices == 8 and lax.axis_size("ta") == 4 and eigs == 64 and columns == 96
    tiles, norm_row = local_tiles(eigvecs, solutions, MASKS if crossed else None)
    slice_times = lax.axis_index("ta") * times + jnp.arange(times, dtype=jnp.int32)
    boundary = jnp.where(slice_times[:, None] < source_times[None, :], -1.0, 1.0).astype(F32)
    chirality = jnp.where(spin_dilution < 2, 1.0, -1.0).astype(F32)
    signs = (boundary[:, :, None] * chirality[None]).reshape(times, pairs)
    if crossed:
        first = lax.broadcasted_iota(jnp.int32, (2 * times, 1, 1), 0) == 0
        norm_row = norm_row + swap(norm_row, 1, 1)
        tail = jnp.where(first, norm_row, 0.0)
        kept, sent = tiles
        held = kept + tail + swap(sent + tail, 0, MASKS[0])
        held = held[0] + swap(held[1], 0, MASKS[1])
        kept, came = held[0], swap(held[1], 0, MASKS[2])
        extra = swap(kept[0] + came[0], 2, 1)
        lanes = jnp.concatenate(
            [signs] * SPINS + [jnp.ones((times, LANES - columns), F32)], 1
        )
        vmem = pl.BlockSpec(memory_space=pltpu.VMEM)
        return pl.pallas_call(
            functools.partial(finish_kernel, cells=cells),
            out_shape=(
                jax.ShapeDtypeStruct((2, times, own_width), F32),
                jax.ShapeDtypeStruct((src_count, col_count), F32),
            ),
            in_specs=[vmem] * 4,
            out_specs=(vmem, vmem),
            compiler_params=pltpu.CompilerParams(vmem_limit_bytes=VMEM_BYTES),
            name="finish",
        )(kept, came, extra, lanes)
    norm_row = lax.psum(norm_row[0, columns : columns + pairs], "sa")
    values = tiles.reshape(eigs // 8, 2, times, 8, LANES)[..., :columns]
    values = values.reshape(eigs // 8, 2, times, 8, SPINS, pairs)
    values = values * signs[None, None, :, None, None]
    values = jnp.transpose(values, (1, 2, 0, 3, 5, 4)).reshape(2, times, devices, own_width)
    values = scatter_sum(jnp.transpose(values, (2, 0, 1, 3)), "sa")
    norms = all_sum(norm_row.reshape(src_count, col_count), "ta") / cells
    return values, norms


def solution(mesh):
    return jax.shard_map(
        on_device,
        mesh=mesh,
        in_specs=(
            P(None, "ta", None, None, "sa"),
            P(None, "ta", None, None, None, None, "sa"),
            P(),
            P(),
        ),
        out_specs=(P(None, "ta", "sa"), P()),
        check_vma=False,
    )
```

```python
import functools

import jax
import jax.numpy as jnp
from jax import lax
from jax.experimental import pallas as pl
from jax.experimental.pallas import tpu as pltpu
from jax.sharding import PartitionSpec as P

F32 = jnp.float32
BF16 = jnp.bfloat16
SPINS = 4
COLORS = 3
LANES = 128
NT_DIMS = (((1,), (1,)), ((), ()))
VMEM_BYTES = 32 * 2**20
MASKS = (1, 3, 5)


def halves(x):
    high = x.astype(BF16)
    return high, (x - high.astype(F32)).astype(BF16)


def dot_nt(a, b, precision=None):
    return lax.dot_general(a, b, NT_DIMS, precision=precision, preferred_element_type=F32)


def split_kernel(s_hbm, split_ref, norm_ref, s_v, sems):
    _, times, pairs, rows, _ = s_hbm.shape
    columns = SPINS * pairs
    blocks = rows // (COLORS * SPINS)
    pitch = s_v.shape[3]
    copies = {}
    for t in range(times):
        for part in range(2):
            copy = pltpu.make_async_copy(
                s_hbm.at[part, t], s_v.at[part, t, :, pl.ds(0, rows)], sems.at[part, t]
            )
            copy.start()
            copies[part, t] = copy
    squares = [jnp.zeros((pairs, LANES), F32) for _ in range(2)]
    for t in range(times):
        for part in range(2):
            copies[part, t].wait()
            flat = s_v.at[part, t].reshape(pairs * pitch, LANES)
            for block in range(COLORS * blocks):
                spins = [
                    flat[pl.ds(block * SPINS + spin, pairs, stride=pitch), :]
                    for spin in range(SPINS)
                ]
                for spin in range(SPINS):
                    squares[spin % 2] = squares[spin % 2] + spins[spin] * spins[spin]
                high, low = halves(jnp.concatenate(spins, 0))
                lanes = slice(block * LANES, (block + 1) * LANES)
                split_ref[t, part * columns : (part + 1) * columns, lanes] = high
                split_ref[t, (2 + part) * columns : (3 + part) * columns, lanes] = low
    placed = jnp.concatenate(
        [
            jnp.zeros((columns, LANES), F32),
            squares[0] + squares[1],
            jnp.zeros((LANES - columns - pairs, LANES), F32),
        ],
        0,
    )
    norm_ref[...] = dot_nt(jnp.ones((8, LANES), F32), placed, lax.Precision.HIGHEST)


def tile_kernel(split_ref, e_ref, *refs, masks):
    _, times, _, eigs, _ = e_ref.shape
    columns = split_ref.shape[1] // 4
    tiles = refs[-1]
    lane = lax.broadcasted_iota(jnp.int32, (columns, LANES), 1)
    for t in range(times):
        wide = []
        for color in range(COLORS):
            stack = jnp.concatenate([e_ref[0, t, color], e_ref[1, t, color]], 0)
            wide.append(jnp.concatenate(halves(stack), 0))
        product = dot_nt(split_ref[t], jnp.concatenate(wide, 1))
        top = product[: 2 * columns]
        joint = top[:, : 2 * eigs] + top[:, 2 * eigs :] + product[2 * columns :, : 2 * eigs]
        real = joint[:columns]
        imag = pltpu.roll(joint[columns:], eigs, 1)
        both = imag + jnp.where(lane < eigs, real, -real)
        both = jnp.concatenate([both, jnp.zeros((LANES - columns, LANES), F32)], 0).T
        both = both.reshape(2, eigs // 8, 8, LANES)
        tiles[:, t] = both[0]
        tiles[:, times + t] = both[1]
    if masks:
        me = lax.axis_index("sa")
        for number, out_ref in enumerate(refs[:2]):
            for high in range(2):
                for low in range(2):
                    mask = number * masks[0] ^ high * masks[1] ^ low * masks[2]
                    out_ref[high, low] = tiles[jnp.bitwise_xor(me, mask)]


def local_tiles(eigvecs, solutions, masks):
    _, times, eigs, _, sites = eigvecs.shape
    pairs = solutions.shape[2] * solutions.shape[3]
    columns = pairs * SPINS
    blocks = sites // LANES
    rows = COLORS * blocks * SPINS
    pitch = rows + 8 if (rows // 8) % 2 == 0 else rows
    e_view = jnp.transpose(eigvecs, (0, 1, 3, 2, 4))
    s_view = jnp.transpose(solutions, (0, 1, 2, 3, 5, 4, 6))
    s_view = s_view.reshape(2, times, pairs, COLORS, SPINS, blocks, LANES)
    s_view = jnp.swapaxes(s_view, 4, 5).reshape(2, times, pairs, rows, LANES)
    s_view = pltpu.with_memory_space_constraint(s_view, pltpu.HBM)
    vmem = pl.BlockSpec(memory_space=pltpu.VMEM)
    params = pltpu.CompilerParams(vmem_limit_bytes=VMEM_BYTES)
    split, norm_row = pl.pallas_call(
        split_kernel,
        out_shape=(
            jax.ShapeDtypeStruct((times, 4 * columns, COLORS * sites), BF16),
            jax.ShapeDtypeStruct((8, LANES), F32),
        ),
        in_specs=[pl.BlockSpec(memory_space=pltpu.HBM)],
        out_specs=(vmem, vmem),
        scratch_shapes=[
            pltpu.VMEM((2, times, pairs, pitch, LANES), F32),
            pltpu.SemaphoreType.DMA((2, times)),
        ],
        compiler_params=params,
        name="split",
        cost_estimate=pl.CostEstimate(
            flops=8 * solutions.size, bytes_accessed=8 * solutions.size, transcendentals=0
        ),
    )(s_view)
    tiles = jax.ShapeDtypeStruct((eigs // 8, 2 * times, 8, LANES), F32)
    block = jax.ShapeDtypeStruct((2, 2, 2 * times, 8, LANES), F32)
    products = pl.pallas_call(
        functools.partial(tile_kernel, masks=masks),
        out_shape=(block, block) if masks else tiles,
        in_specs=[vmem] * 2,
        out_specs=(vmem, vmem) if masks else vmem,
        scratch_shapes=[pltpu.VMEM(tiles.shape, F32)] if masks else [],
        compiler_params=params,
        name="tiles",
        cost_estimate=pl.CostEstimate(
            flops=24 * times * eigs * columns * COLORS * sites,
            bytes_accessed=4 * (eigvecs.size + solutions.size),
            transcendentals=0,
        ),
    )(split, e_view)
    return products, norm_row


def finish_kernel(kept_ref, came_ref, sign_ref, out_ref, norm_ref, *, cells):
    _, times, width = out_ref.shape
    src_count, col_count = norm_ref.shape
    columns = width // 8
    pairs = columns // SPINS
    row = lax.broadcasted_iota(jnp.int32, (8, LANES), 0)
    lane = lax.broadcasted_iota(jnp.int32, (8, LANES), 1)
    column = jnp.bitwise_and(lane + LANES - (row * columns) % LANES, LANES - 1)
    source = jnp.where(column < columns, (column % SPINS) * pairs + column // SPINS, 0)
    for part in range(2):
        for t in range(times):
            index = part * times + t
            tile = kept_ref[index] + came_ref[index]
            if index == 0:
                for src in range(src_count):
                    shift = 2 * LANES - columns - src * col_count
                    norm = pltpu.roll(tile, shift % LANES, 1)
                    norm_ref[src : src + 1, :] = norm[:1, :col_count] / cells
            tile = tile * sign_ref[t : t + 1, :]
            tile = jnp.take_along_axis(tile, source, axis=1)
            for piece in range(width // LANES):
                first = piece * LANES // columns
                edge = (first + 1) * columns - piece * LANES
                out_ref[part, t : t + 1, piece * LANES : (piece + 1) * LANES] = jnp.where(
                    lane[:1] < edge, tile[first : first + 1], tile[first + 1 : first + 2]
                )


def swap(x, ta_mask, sa_mask):
    ta_size, sa_size = lax.axis_size("ta"), lax.axis_size("sa")
    pairs = [
        (ta * sa_size + sa, (ta ^ ta_mask) * sa_size + (sa ^ sa_mask))
        for ta in range(ta_size)
        for sa in range(sa_size)
    ]
    return lax.ppermute(x, ("ta", "sa"), pairs)


def radices_of(count):
    found = []
    for prime in (2, 3, 5, 7, 11, 13):
        while count % prime == 0:
            found.append(prime)
            count //= prime
    return found + ([count] if count > 1 else [])


def shifted(size, weight, radix, shift):
    moves = []
    for source in range(size):
        own = (source // weight) % radix
        moves.append((source, source + ((own + shift) % radix - own) * weight))
    return moves


def scatter_sum(blocks, axis):
    size = lax.axis_size(axis)
    me = lax.axis_index(axis)
    radices = radices_of(size)
    held = blocks.reshape(tuple(reversed(radices)) + blocks.shape[1:])
    weight = 1
    for depth, radix in enumerate(radices):
        dim = len(radices) - 1 - depth
        digit = (me // weight) % radix
        total = lax.dynamic_index_in_dim(held, digit, dim, False)
        for shift in range(1, radix):
            send = lax.dynamic_index_in_dim(held, (digit + shift) % radix, dim, False)
            total = total + lax.ppermute(send, axis, shifted(size, weight, radix, shift))
        held = total
        weight *= radix
    return held


def all_sum(x, axis):
    size = lax.axis_size(axis)
    weight = 1
    for radix in radices_of(size):
        total = x
        for shift in range(1, radix):
            total = total + lax.ppermute(x, axis, shifted(size, weight, radix, shift))
        x = total
        weight *= radix
    return x


def on_device(eigvecs, solutions, source_times, spin_dilution):
    _, times, eigs, _, sites = eigvecs.shape
    src_count, col_count = spin_dilution.shape
    pairs = src_count * col_count
    columns = pairs * SPINS
    devices = lax.axis_size("sa")
    cells = 12.0 * times * lax.axis_size("ta") * sites * devices
    own_width = eigs * columns // devices

    crossed = devices == 8 and lax.axis_size("ta") == 4 and eigs == 64 and columns == 96
    tiles, norm_row = local_tiles(eigvecs, solutions, MASKS if crossed else None)
    slice_times = lax.axis_index("ta") * times + jnp.arange(times, dtype=jnp.int32)
    boundary = jnp.where(slice_times[:, None] < source_times[None, :], -1.0, 1.0).astype(F32)
    chirality = jnp.where(spin_dilution < 2, 1.0, -1.0).astype(F32)
    signs = (boundary[:, :, None] * chirality[None]).reshape(times, pairs)
    if crossed:
        first = lax.broadcasted_iota(jnp.int32, (2 * times, 1, 1), 0) == 0
        norm_row = norm_row + swap(norm_row, 1, 1) + swap(norm_row, 2, 1) + swap(norm_row, 3, 1)
        tail = jnp.where(first, norm_row, 0.0)
        kept, sent = tiles
        held = kept + tail + swap(sent + tail, 0, MASKS[0])
        held = held[0] + swap(held[1], 0, MASKS[1])
        kept, came = held[0], swap(held[1], 0, MASKS[2])
        lanes = jnp.concatenate(
            [signs] * SPINS + [jnp.ones((times, LANES - columns), F32)], 1
        )
        vmem = pl.BlockSpec(memory_space=pltpu.VMEM)
        return pl.pallas_call(
            functools.partial(finish_kernel, cells=cells),
            out_shape=(
                jax.ShapeDtypeStruct((2, times, own_width), F32),
                jax.ShapeDtypeStruct((src_count, col_count), F32),
            ),
            in_specs=[vmem] * 3,
            out_specs=(vmem, vmem),
            compiler_params=pltpu.CompilerParams(vmem_limit_bytes=VMEM_BYTES),
            name="finish",
        )(kept, came, lanes)
    norm_row = lax.psum(norm_row[0, columns : columns + pairs], "sa")
    values = tiles.reshape(eigs // 8, 2, times, 8, LANES)[..., :columns]
    values = values.reshape(eigs // 8, 2, times, 8, SPINS, pairs)
    values = values * signs[None, None, :, None, None]
    values = jnp.transpose(values, (1, 2, 0, 3, 5, 4)).reshape(2, times, devices, own_width)
    values = scatter_sum(jnp.transpose(values, (2, 0, 1, 3)), "sa")
    norms = all_sum(norm_row.reshape(src_count, col_count), "ta") / cells
    return values, norms


def solution(mesh):
    return jax.shard_map(
        on_device,
        mesh=mesh,
        in_specs=(
            P(None, "ta", None, None, "sa"),
            P(None, "ta", None, None, None, None, "sa"),
            P(),
            P(),
        ),
        out_specs=(P(None, "ta", "sa"), P()),
        check_vma=False,
    )
```

```python
import functools

import jax
import jax.numpy as jnp
from jax import lax
from jax.experimental import pallas as pl
from jax.experimental.pallas import tpu as pltpu
from jax.sharding import PartitionSpec as P


F32 = jnp.float32
BF16 = jnp.bfloat16
SPINS = 4
COLORS = 3
LANES = 128
NT_DIMS = (((1,), (1,)), ((), ()))
VMEM_BYTES = 32 * 2**20
MASKS = (1, 3, 5)


def halves(x):
    high = x.astype(BF16)
    return high, (x - high.astype(F32)).astype(BF16)


def dot_nt(a, b, precision=None):
    return lax.dot_general(a, b, NT_DIMS, precision=precision, preferred_element_type=F32)


def split_kernel(s_hbm, split_ref, norm_ref, s_v, sems):
    _, times, pairs, rows, _ = s_hbm.shape
    columns = SPINS * pairs
    blocks = rows // (COLORS * SPINS)
    pitch = s_v.shape[3]
    copies = {}
    for t in range(times):
        for part in range(2):
            copy = pltpu.make_async_copy(
                s_hbm.at[part, t], s_v.at[part, t, :, pl.ds(0, rows)], sems.at[part, t]
            )
            copy.start()
            copies[part, t] = copy
    squares = [jnp.zeros((pairs, LANES), F32) for _ in range(2)]
    for t in range(times):
        for part in range(2):
            copies[part, t].wait()
            flat = s_v.at[part, t].reshape(pairs * pitch, LANES)
            for block in range(COLORS * blocks):
                spins = [
                    flat[pl.ds(block * SPINS + spin, pairs, stride=pitch), :]
                    for spin in range(SPINS)
                ]
                for spin in range(SPINS):
                    squares[spin % 2] = squares[spin % 2] + spins[spin] * spins[spin]
                high, low = halves(jnp.concatenate(spins, 0))
                lanes = slice(block * LANES, (block + 1) * LANES)
                split_ref[t, part * columns : (part + 1) * columns, lanes] = high
                split_ref[t, (2 + part) * columns : (3 + part) * columns, lanes] = low
    placed = jnp.concatenate(
        [
            jnp.zeros((columns, LANES), F32),
            squares[0] + squares[1],
            jnp.zeros((LANES - columns - pairs, LANES), F32),
        ],
        0,
    )
    norm_ref[...] = dot_nt(jnp.ones((8, LANES), F32), placed, lax.Precision.HIGHEST)


def tile_kernel(split_ref, e_ref, *refs, masks):
    _, times, _, eigs, _ = e_ref.shape
    columns = split_ref.shape[1] // 4
    tiles = refs[-1]
    lane = lax.broadcasted_iota(jnp.int32, (columns, LANES), 1)
    for t in range(times):
        wide = []
        for color in range(COLORS):
            stack = jnp.concatenate([e_ref[0, t, color], e_ref[1, t, color]], 0)
            wide.append(jnp.concatenate(halves(stack), 0))
        product = dot_nt(split_ref[t], jnp.concatenate(wide, 1))
        top = product[: 2 * columns]
        joint = top[:, : 2 * eigs] + top[:, 2 * eigs :] + product[2 * columns :, : 2 * eigs]
        real = joint[:columns]
        imag = pltpu.roll(joint[columns:], eigs, 1)
        both = imag + jnp.where(lane < eigs, real, -real)
        both = jnp.concatenate([both, jnp.zeros((LANES - columns, LANES), F32)], 0).T
        both = both.reshape(2, eigs // 8, 8, LANES)
        tiles[:, t] = both[0]
        tiles[:, times + t] = both[1]
    if masks:
        me = lax.axis_index("sa")
        for number, out_ref in enumerate(refs[:2]):
            for high in range(2):
                for low in range(2):
                    mask = number * masks[0] ^ high * masks[1] ^ low * masks[2]
                    out_ref[high, low] = tiles[jnp.bitwise_xor(me, mask)]


def local_tiles(eigvecs, solutions, masks):
    _, times, eigs, _, sites = eigvecs.shape
    pairs = solutions.shape[2] * solutions.shape[3]
    columns = pairs * SPINS
    blocks = sites // LANES
    rows = COLORS * blocks * SPINS
    pitch = rows + 8 if (rows // 8) % 2 == 0 else rows
    e_view = jnp.transpose(eigvecs, (0, 1, 3, 2, 4))
    s_view = jnp.transpose(solutions, (0, 1, 2, 3, 5, 4, 6))
    s_view = s_view.reshape(2, times, pairs, COLORS, SPINS, blocks, LANES)
    s_view = jnp.swapaxes(s_view, 4, 5).reshape(2, times, pairs, rows, LANES)
    s_view = pltpu.with_memory_space_constraint(s_view, pltpu.HBM)
    vmem = pl.BlockSpec(memory_space=pltpu.VMEM)
    params = pltpu.CompilerParams(vmem_limit_bytes=VMEM_BYTES)
    split, norm_row = pl.pallas_call(
        split_kernel,
        out_shape=(
            jax.ShapeDtypeStruct((times, 4 * columns, COLORS * sites), BF16),
            jax.ShapeDtypeStruct((8, LANES), F32),
        ),
        in_specs=[pl.BlockSpec(memory_space=pltpu.HBM)],
        out_specs=(vmem, vmem),
        scratch_shapes=[
            pltpu.VMEM((2, times, pairs, pitch, LANES), F32),
            pltpu.SemaphoreType.DMA((2, times)),
        ],
        compiler_params=params,
        name="split",
        cost_estimate=pl.CostEstimate(
            flops=8 * solutions.size, bytes_accessed=8 * solutions.size, transcendentals=0
        ),
    )(s_view)
    tiles = jax.ShapeDtypeStruct((eigs // 8, 2 * times, 8, LANES), F32)
    block = jax.ShapeDtypeStruct((2, 2, 2 * times, 8, LANES), F32)
    make_tiles = pl.pallas_call(
        functools.partial(tile_kernel, masks=masks),
        out_shape=(block, block) if masks else tiles,
        in_specs=[vmem] * 2,
        out_specs=(vmem, vmem) if masks else vmem,
        scratch_shapes=[pltpu.VMEM(tiles.shape, F32)] if masks else [],
        compiler_params=params,
        name="tiles",
        cost_estimate=pl.CostEstimate(
            flops=24 * times * eigs * columns * COLORS * sites,
            bytes_accessed=4 * (eigvecs.size + solutions.size),
            transcendentals=0,
        ),
    )
    products = make_tiles(split, e_view)
    return products, norm_row


def finish_kernel(kept_ref, came_ref, sign_ref, out_ref):
    _, times, width = out_ref.shape
    columns = width // 8
    pairs = columns // SPINS
    row = lax.broadcasted_iota(jnp.int32, (8, LANES), 0)
    lane = lax.broadcasted_iota(jnp.int32, (8, LANES), 1)
    column = jnp.bitwise_and(lane + LANES - (row * columns) % LANES, LANES - 1)
    source = jnp.where(column < columns, (column % SPINS) * pairs + column // SPINS, 0)
    for part in range(2):
        for t in range(times):
            index = part * times + t
            tile = (kept_ref[index] + came_ref[index]) * sign_ref[t : t + 1, :]
            tile = jnp.take_along_axis(tile, source, axis=1)
            for piece in range(width // LANES):
                first = piece * LANES // columns
                edge = (first + 1) * columns - piece * LANES
                out_ref[part, t : t + 1, piece * LANES : (piece + 1) * LANES] = jnp.where(
                    lane[:1] < edge, tile[first : first + 1], tile[first + 1 : first + 2]
                )


def norm_kernel(kept_ref, extra_ref, norm_ref, *, first, cells):
    src_count, col_count = norm_ref.shape
    total = kept_ref[...] + extra_ref[...]
    for src in range(src_count):
        shift = 2 * LANES - first - src * col_count
        norm = pltpu.roll(total, shift % LANES, 1)
        norm_ref[src : src + 1, :] = norm[:1, :col_count] / cells


def swap(x, ta_mask, sa_mask):
    ta_size, sa_size = lax.axis_size("ta"), lax.axis_size("sa")
    pairs = [
        (ta * sa_size + sa, (ta ^ ta_mask) * sa_size + (sa ^ sa_mask))
        for ta in range(ta_size)
        for sa in range(sa_size)
    ]
    return lax.ppermute(x, ("ta", "sa"), pairs)


def radices_of(count):
    found = []
    for prime in (2, 3, 5, 7, 11, 13):
        while count % prime == 0:
            found.append(prime)
            count //= prime
    return found + ([count] if count > 1 else [])


def shifted(size, weight, radix, shift):
    moves = []
    for source in range(size):
        own = (source // weight) % radix
        moves.append((source, source + ((own + shift) % radix - own) * weight))
    return moves


def scatter_sum(blocks, axis):
    size = lax.axis_size(axis)
    me = lax.axis_index(axis)
    radices = radices_of(size)
    held = blocks.reshape(tuple(reversed(radices)) + blocks.shape[1:])
    weight = 1
    for depth, radix in enumerate(radices):
        dim = len(radices) - 1 - depth
        digit = (me // weight) % radix
        total = lax.dynamic_index_in_dim(held, digit, dim, False)
        for shift in range(1, radix):
            send = lax.dynamic_index_in_dim(held, (digit + shift) % radix, dim, False)
            total = total + lax.ppermute(send, axis, shifted(size, weight, radix, shift))
        held = total
        weight *= radix
    return held


def all_sum(x, axis):
    size = lax.axis_size(axis)
    weight = 1
    for radix in radices_of(size):
        total = x
        for shift in range(1, radix):
            total = total + lax.ppermute(x, axis, shifted(size, weight, radix, shift))
        x = total
        weight *= radix
    return x


def on_device(eigvecs, solutions, source_times, spin_dilution):
    _, times, eigs, _, sites = eigvecs.shape
    src_count, col_count = spin_dilution.shape
    pairs = src_count * col_count
    columns = pairs * SPINS
    devices = lax.axis_size("sa")
    cells = 12.0 * times * lax.axis_size("ta") * sites * devices
    own_width = eigs * columns // devices

    crossed = devices == 8 and lax.axis_size("ta") == 4 and eigs == 64 and columns == 96
    tiles, norm_row = local_tiles(eigvecs, solutions, MASKS if crossed else None)
    slice_times = lax.axis_index("ta") * times + jnp.arange(times, dtype=jnp.int32)
    boundary = jnp.where(slice_times[:, None] < source_times[None, :], -1.0, 1.0).astype(F32)
    chirality = jnp.where(spin_dilution < 2, 1.0, -1.0).astype(F32)
    signs = (boundary[:, :, None] * chirality[None]).reshape(times, pairs)
    if crossed:
        first = lax.broadcasted_iota(jnp.int32, (2 * times, 1, 1), 0) == 0
        own = norm_row
        for ta_mask in (1, 2, 3):
            norm_row = norm_row + swap(own, ta_mask, 1)
        kept, sent = tiles
        held = kept + swap(sent, 0, MASKS[0]) + jnp.where(first, norm_row, 0.0)
        held = held[0] + swap(held[1], 0, MASKS[1])
        kept, came = held[0], swap(held[1], 0, MASKS[2])
        line = kept[0] + came[0]
        extra = swap(line, 0, 1)
        lanes = jnp.concatenate(
            [signs] * SPINS + [jnp.ones((times, LANES - columns), F32)], 1
        )
        vmem = pl.BlockSpec(memory_space=pltpu.VMEM)
        params = pltpu.CompilerParams(vmem_limit_bytes=VMEM_BYTES)
        values = pl.pallas_call(
            finish_kernel,
            out_shape=jax.ShapeDtypeStruct((2, times, own_width), F32),
            in_specs=[vmem] * 3,
            out_specs=vmem,
            compiler_params=params,
            name="finish",
            cost_estimate=pl.CostEstimate(flops=10**7, bytes_accessed=10**6, transcendentals=0),
        )(kept, came, lanes)
        norms = pl.pallas_call(
            functools.partial(norm_kernel, first=columns, cells=cells),
            out_shape=jax.ShapeDtypeStruct((src_count, col_count), F32),
            in_specs=[vmem] * 2,
            out_specs=vmem,
            compiler_params=params,
            name="norms",
        )(line, extra)
        return values, norms
    norm_row = lax.psum(norm_row[0, columns : columns + pairs], "sa")
    values = tiles.reshape(eigs // 8, 2, times, 8, LANES)[..., :columns]
    values = values.reshape(eigs // 8, 2, times, 8, SPINS, pairs)
    values = values * signs[None, None, :, None, None]
    values = jnp.transpose(values, (1, 2, 0, 3, 5, 4)).reshape(2, times, devices, own_width)
    values = scatter_sum(jnp.transpose(values, (2, 0, 1, 3)), "sa")
    norms = all_sum(norm_row.reshape(src_count, col_count), "ta") / cells
    return values, norms


def solution(mesh):
    return jax.shard_map(
        on_device,
        mesh=mesh,
        in_specs=(
            P(None, "ta", None, None, "sa"),
            P(None, "ta", None, None, None, None, "sa"),
            P(),
            P(),
        ),
        out_specs=(P(None, "ta", "sa"), P()),
        check_vma=False,
    )
```

```python
import functools

import jax
import jax.numpy as jnp
from jax import lax
from jax.experimental import pallas as pl
from jax.experimental.pallas import tpu as pltpu
from jax.sharding import PartitionSpec as P


F32 = jnp.float32
BF16 = jnp.bfloat16
SPINS = 4
COLORS = 3
LANES = 128
NT_DIMS = (((1,), (1,)), ((), ()))
VMEM_BYTES = 32 * 2**20
MASKS = (1, 3, 5)


def halves(x):
    high = x.astype(BF16)
    return high, (x - high.astype(F32)).astype(BF16)


def dot_nt(a, b, precision=None):
    return lax.dot_general(a, b, NT_DIMS, precision=precision, preferred_element_type=F32)


def split_kernel(s_hbm, split_ref, sums_ref, s_v, sems):
    _, times, pairs, rows, _ = s_hbm.shape
    columns = SPINS * pairs
    pitch = s_v.shape[3]
    chunk = rows // COLORS
    copies = []
    for t in range(times):
        for part in range(2):
            for color in range(COLORS):
                here = pl.ds(color * chunk, chunk)
                copy = pltpu.make_async_copy(
                    s_hbm.at[part, t, :, here],
                    s_v.at[part, t, :, here],
                    sems.at[part, t, color],
                )
                copy.start()
                copies.append((t, part, color, copy))
    squares = [jnp.zeros((pairs, LANES), F32) for _ in range(SPINS)]
    for t, part, color, copy in copies:
        copy.wait()
        flat = s_v.at[part, t].reshape(pairs * pitch, LANES)
        for block in range(color * chunk // SPINS, (color + 1) * chunk // SPINS):
            spins = [
                flat[pl.ds(block * SPINS + spin, pairs, stride=pitch), :]
                for spin in range(SPINS)
            ]
            for spin in range(SPINS):
                squares[spin] = squares[spin] + spins[spin] * spins[spin]
            high, low = halves(jnp.concatenate(spins, 0))
            split_ref[t, block, part * columns : (part + 1) * columns] = high
            split_ref[t, block, (2 + part) * columns : (3 + part) * columns] = low
    sums_ref[...] = (squares[0] + squares[1]) + (squares[2] + squares[3])


def row_kernel(sums_ref, row_ref, *, columns):
    pairs = sums_ref.shape[0]
    placed = jnp.concatenate(
        [
            jnp.zeros((columns, LANES), F32),
            sums_ref[...],
            jnp.zeros((LANES - columns - pairs, LANES), F32),
        ],
        0,
    )
    high, low = halves(placed)
    total = dot_nt(jnp.ones((16, 2 * LANES), BF16), jnp.concatenate([high, low], 1))
    row_ref[...] = total[:8]


def tile_kernel(split_ref, e_ref, *refs, masks):
    _, times, _, eigs, _ = e_ref.shape
    columns = split_ref.shape[2] // 4
    blocks = split_ref.shape[1]
    tiles = refs[-1]
    lane = lax.broadcasted_iota(jnp.int32, (columns, LANES), 1)
    for t in range(times):
        wide = []
        for color in range(COLORS):
            stack = jnp.concatenate([e_ref[0, t, color], e_ref[1, t, color]], 0)
            wide.append(jnp.concatenate(halves(stack), 0))
        left = jnp.concatenate([split_ref[t, block] for block in range(blocks)], 1)
        product = dot_nt(left, jnp.concatenate(wide, 1))
        top = product[: 2 * columns]
        joint = top[:, : 2 * eigs] + top[:, 2 * eigs :] + product[2 * columns :, : 2 * eigs]
        joint = joint + product[2 * columns :, 2 * eigs :]
        real = joint[:columns]
        imag = pltpu.roll(joint[columns:], eigs, 1)
        both = imag + jnp.where(lane < eigs, real, -real)
        both = jnp.concatenate([both, jnp.zeros((LANES - columns, LANES), F32)], 0).T
        both = both.reshape(2, eigs // 8, 8, LANES)
        tiles[:, t] = both[0]
        tiles[:, times + t] = both[1]
    if masks:
        me = lax.axis_index("sa")
        for number, out_ref in enumerate(refs[:2]):
            for high in range(2):
                for low in range(2):
                    mask = number * masks[0] ^ high * masks[1] ^ low * masks[2]
                    out_ref[high, low] = tiles[jnp.bitwise_xor(me, mask)]


def local_tiles(eigvecs, solutions, masks):
    _, times, eigs, _, sites = eigvecs.shape
    pairs = solutions.shape[2] * solutions.shape[3]
    columns = pairs * SPINS
    blocks = sites // LANES
    rows = COLORS * blocks * SPINS
    pitch = rows + 8 if (rows // 8) % 2 == 0 else rows
    e_view = jnp.transpose(eigvecs, (0, 1, 3, 2, 4))
    s_view = jnp.transpose(solutions, (0, 1, 2, 3, 5, 4, 6))
    s_view = s_view.reshape(2, times, pairs, COLORS, SPINS, blocks, LANES)
    s_view = jnp.swapaxes(s_view, 4, 5).reshape(2, times, pairs, rows, LANES)
    s_view = pltpu.with_memory_space_constraint(s_view, pltpu.HBM)
    vmem = pl.BlockSpec(memory_space=pltpu.VMEM)
    params = pltpu.CompilerParams(vmem_limit_bytes=VMEM_BYTES)
    split, sums = pl.pallas_call(
        split_kernel,
        out_shape=(
            jax.ShapeDtypeStruct((times, COLORS * blocks, 4 * columns, LANES), BF16),
            jax.ShapeDtypeStruct((pairs, LANES), F32),
        ),
        in_specs=[pl.BlockSpec(memory_space=pltpu.HBM)],
        out_specs=(vmem, vmem),
        scratch_shapes=[
            pltpu.VMEM((2, times, pairs, pitch, LANES), F32),
            pltpu.SemaphoreType.DMA((2, times, COLORS)),
        ],
        compiler_params=params,
        name="split",
        cost_estimate=pl.CostEstimate(
            flops=solutions.size, bytes_accessed=8 * solutions.size, transcendentals=0
        ),
    )(s_view)
    norm_row = pl.pallas_call(
        functools.partial(row_kernel, columns=columns),
        out_shape=jax.ShapeDtypeStruct((8, LANES), F32),
        in_specs=[vmem],
        out_specs=vmem,
        compiler_params=params,
        name="row",
        cost_estimate=pl.CostEstimate(flops=10**9, bytes_accessed=10**7, transcendentals=0),
    )(sums)
    tiles = jax.ShapeDtypeStruct((eigs // 8, 2 * times, 8, LANES), F32)
    block = jax.ShapeDtypeStruct((2, 2, 2 * times, 8, LANES), F32)
    make_tiles = pl.pallas_call(
        functools.partial(tile_kernel, masks=masks),
        out_shape=(block, block) if masks else tiles,
        in_specs=[vmem] * 2,
        out_specs=(vmem, vmem) if masks else vmem,
        scratch_shapes=[pltpu.VMEM(tiles.shape, F32)] if masks else [],
        compiler_params=params,
        name="tiles",
        cost_estimate=pl.CostEstimate(
            flops=24 * times * eigs * columns * COLORS * sites,
            bytes_accessed=4 * (eigvecs.size + solutions.size),
            transcendentals=0,
        ),
    )
    products = make_tiles(split, e_view)
    return products, norm_row


def finish_kernel(kept_ref, came_ref, sign_ref, out_ref):
    _, times, width = out_ref.shape
    columns = width // 8
    pairs = columns // SPINS
    row = lax.broadcasted_iota(jnp.int32, (8, LANES), 0)
    lane = lax.broadcasted_iota(jnp.int32, (8, LANES), 1)
    column = jnp.bitwise_and(lane + LANES - (row * columns) % LANES, LANES - 1)
    source = jnp.where(column < columns, (column % SPINS) * pairs + column // SPINS, 0)
    for part in range(2):
        for t in range(times):
            index = part * times + t
            tile = (kept_ref[index] + came_ref[index]) * sign_ref[t : t + 1, :]
            tile = jnp.take_along_axis(tile, source, axis=1)
            for piece in range(width // LANES):
                first = piece * LANES // columns
                edge = (first + 1) * columns - piece * LANES
                out_ref[part, t : t + 1, piece * LANES : (piece + 1) * LANES] = jnp.where(
                    lane[:1] < edge, tile[first : first + 1], tile[first + 1 : first + 2]
                )


def norm_kernel(kept_ref, extra_ref, norm_ref, *, first, cells):
    src_count, col_count = norm_ref.shape
    total = kept_ref[...] + extra_ref[...]
    for src in range(src_count):
        shift = 2 * LANES - first - src * col_count
        norm = pltpu.roll(total, shift % LANES, 1)
        norm_ref[src : src + 1, :] = norm[:1, :col_count] / cells


def swap(x, ta_mask, sa_mask):
    ta_size, sa_size = lax.axis_size("ta"), lax.axis_size("sa")
    pairs = [
        (ta * sa_size + sa, (ta ^ ta_mask) * sa_size + (sa ^ sa_mask))
        for ta in range(ta_size)
        for sa in range(sa_size)
    ]
    return lax.ppermute(x, ("ta", "sa"), pairs)


def radices_of(count):
    found = []
    for prime in (2, 3, 5, 7, 11, 13):
        while count % prime == 0:
            found.append(prime)
            count //= prime
    return found + ([count] if count > 1 else [])


def shifted(size, weight, radix, shift):
    moves = []
    for source in range(size):
        own = (source // weight) % radix
        moves.append((source, source + ((own + shift) % radix - own) * weight))
    return moves


def scatter_sum(blocks, axis):
    size = lax.axis_size(axis)
    me = lax.axis_index(axis)
    radices = radices_of(size)
    held = blocks.reshape(tuple(reversed(radices)) + blocks.shape[1:])
    weight = 1
    for depth, radix in enumerate(radices):
        dim = len(radices) - 1 - depth
        digit = (me // weight) % radix
        total = lax.dynamic_index_in_dim(held, digit, dim, False)
        for shift in range(1, radix):
            send = lax.dynamic_index_in_dim(held, (digit + shift) % radix, dim, False)
            total = total + lax.ppermute(send, axis, shifted(size, weight, radix, shift))
        held = total
        weight *= radix
    return held


def all_sum(x, axis):
    size = lax.axis_size(axis)
    weight = 1
    for radix in radices_of(size):
        total = x
        for shift in range(1, radix):
            total = total + lax.ppermute(x, axis, shifted(size, weight, radix, shift))
        x = total
        weight *= radix
    return x


def on_device(eigvecs, solutions, source_times, spin_dilution):
    _, times, eigs, _, sites = eigvecs.shape
    src_count, col_count = spin_dilution.shape
    pairs = src_count * col_count
    columns = pairs * SPINS
    devices = lax.axis_size("sa")
    cells = 12.0 * times * lax.axis_size("ta") * sites * devices
    own_width = eigs * columns // devices

    crossed = devices == 8 and lax.axis_size("ta") == 4 and eigs == 64 and columns == 96
    tiles, norm_row = local_tiles(eigvecs, solutions, MASKS if crossed else None)
    slice_times = lax.axis_index("ta") * times + jnp.arange(times, dtype=jnp.int32)
    boundary = jnp.where(slice_times[:, None] < source_times[None, :], -1.0, 1.0).astype(F32)
    chirality = jnp.where(spin_dilution < 2, 1.0, -1.0).astype(F32)
    signs = (boundary[:, :, None] * chirality[None]).reshape(times, pairs)
    if crossed:
        first = lax.broadcasted_iota(jnp.int32, (2 * times, 1, 1), 0) == 0
        norm_row = norm_row + swap(norm_row, 1, 1)
        norm_row = norm_row + swap(norm_row, 2, 1)
        kept, sent = tiles
        held = kept + swap(sent, 0, MASKS[0]) + jnp.where(first, norm_row, 0.0)
        held = held[0] + swap(held[1], 0, MASKS[1])
        kept, came = held[0], swap(held[1], 0, MASKS[2])
        line = kept[0] + came[0]
        extra = swap(line, 0, 1)
        lanes = jnp.concatenate(
            [signs] * SPINS + [jnp.ones((times, LANES - columns), F32)], 1
        )
        vmem = pl.BlockSpec(memory_space=pltpu.VMEM)
        params = pltpu.CompilerParams(vmem_limit_bytes=VMEM_BYTES)
        values = pl.pallas_call(
            finish_kernel,
            out_shape=jax.ShapeDtypeStruct((2, times, own_width), F32),
            in_specs=[vmem] * 3,
            out_specs=vmem,
            compiler_params=params,
            name="finish",
            cost_estimate=pl.CostEstimate(flops=10**7, bytes_accessed=10**6, transcendentals=0),
        )(kept, came, lanes)
        norms = pl.pallas_call(
            functools.partial(norm_kernel, first=columns, cells=cells),
            out_shape=jax.ShapeDtypeStruct((src_count, col_count), F32),
            in_specs=[vmem] * 2,
            out_specs=vmem,
            compiler_params=params,
            name="norms",
        )(line, extra)
        return values, norms
    norm_row = lax.psum(norm_row[0, columns : columns + pairs], "sa")
    values = tiles.reshape(eigs // 8, 2, times, 8, LANES)[..., :columns]
    values = values.reshape(eigs // 8, 2, times, 8, SPINS, pairs)
    values = values * signs[None, None, :, None, None]
    values = jnp.transpose(values, (1, 2, 0, 3, 5, 4)).reshape(2, times, devices, own_width)
    values = scatter_sum(jnp.transpose(values, (2, 0, 1, 3)), "sa")
    norms = all_sum(norm_row.reshape(src_count, col_count), "ta") / cells
    return values, norms


def solution(mesh):
    return jax.shard_map(
        on_device,
        mesh=mesh,
        in_specs=(
            P(None, "ta", None, None, "sa"),
            P(None, "ta", None, None, None, None, "sa"),
            P(),
            P(),
        ),
        out_specs=(P(None, "ta", "sa"), P()),
        check_vma=False,
    )
```

```python
import functools

import jax
import jax.numpy as jnp
from jax import lax
from jax.experimental import pallas as pl
from jax.experimental.pallas import tpu as pltpu
from jax.sharding import PartitionSpec as P


F32 = jnp.float32
BF16 = jnp.bfloat16
SPINS = 4
COLORS = 3
LANES = 128
NT_DIMS = (((1,), (1,)), ((), ()))
VMEM_BYTES = 32 * 2**20
MASKS = (1, 3, 5)


def halves(x):
    high = x.astype(BF16)
    return high, (x - high.astype(F32)).astype(BF16)


def dot_nt(a, b, precision=None):
    return lax.dot_general(a, b, NT_DIMS, precision=precision, preferred_element_type=F32)


def split_kernel(s_hbm, split_ref, sums_ref, s_v, sems):
    _, times, pairs, rows, _ = s_hbm.shape
    columns = SPINS * pairs
    pitch = s_v.shape[3]
    chunk = rows // COLORS
    copies = []
    for t in range(times):
        for part in range(2):
            for color in range(COLORS):
                here = pl.ds(color * chunk, chunk)
                copy = pltpu.make_async_copy(
                    s_hbm.at[part, t, :, here],
                    s_v.at[part, t, :, here],
                    sems.at[part, t, color],
                )
                copy.start()
                copies.append((t, part, color, copy))
    squares = [jnp.zeros((pairs, LANES), F32) for _ in range(SPINS)]
    for t, part, color, copy in copies:
        copy.wait()
        flat = s_v.at[part, t].reshape(pairs * pitch, LANES)
        for block in range(color * chunk // SPINS, (color + 1) * chunk // SPINS):
            spins = [
                flat[pl.ds(block * SPINS + spin, pairs, stride=pitch), :]
                for spin in range(SPINS)
            ]
            for spin in range(SPINS):
                squares[spin] = squares[spin] + spins[spin] * spins[spin]
            high, low = halves(jnp.concatenate(spins, 0))
            split_ref[t, block, part * columns : (part + 1) * columns] = high
            split_ref[t, block, (2 + part) * columns : (3 + part) * columns] = low
    sums_ref[...] = (squares[0] + squares[1]) + (squares[2] + squares[3])


def row_kernel(sums_ref, row_ref, *, columns):
    pairs = sums_ref.shape[0]
    placed = jnp.concatenate(
        [
            jnp.zeros((columns, LANES), F32),
            sums_ref[...],
            jnp.zeros((LANES - columns - pairs, LANES), F32),
        ],
        0,
    )
    high, low = halves(placed)
    total = dot_nt(jnp.ones((16, 2 * LANES), BF16), jnp.concatenate([high, low], 1))
    row_ref[...] = total[:8]


def tile_kernel(split_ref, e_ref, *refs, masks):
    _, times, _, eigs, _ = e_ref.shape
    columns = split_ref.shape[2] // 4
    blocks = split_ref.shape[1]
    tiles = refs[-1]
    lane = lax.broadcasted_iota(jnp.int32, (columns, LANES), 1)
    for t in range(times):
        wide = []
        for color in range(COLORS):
            stack = jnp.concatenate([e_ref[0, t, color], e_ref[1, t, color]], 0)
            wide.append(jnp.concatenate(halves(stack), 0))
        left = jnp.concatenate([split_ref[t, block] for block in range(blocks)], 1)
        product = dot_nt(left, jnp.concatenate(wide, 1))
        top = product[: 2 * columns]
        joint = top[:, : 2 * eigs] + top[:, 2 * eigs :] + product[2 * columns :, : 2 * eigs]
        joint = joint + product[2 * columns :, 2 * eigs :]
        real = joint[:columns]
        imag = pltpu.roll(joint[columns:], eigs, 1)
        both = imag + jnp.where(lane < eigs, real, -real)
        both = jnp.concatenate([both, jnp.zeros((LANES - columns, LANES), F32)], 0).T
        both = both.reshape(2, eigs // 8, 8, LANES)
        tiles[:, t] = both[0]
        tiles[:, times + t] = both[1]
    if masks:
        me = lax.axis_index("sa")
        for number, out_ref in enumerate(refs[:2]):
            for high in range(2):
                for low in range(2):
                    mask = number * masks[0] ^ high * masks[1] ^ low * masks[2]
                    out_ref[high, low] = tiles[jnp.bitwise_xor(me, mask)]


def local_tiles(eigvecs, solutions, masks):
    _, times, eigs, _, sites = eigvecs.shape
    pairs = solutions.shape[2] * solutions.shape[3]
    columns = pairs * SPINS
    blocks = sites // LANES
    rows = COLORS * blocks * SPINS
    pitch = rows + 8 if (rows // 8) % 2 == 0 else rows
    e_view = jnp.transpose(eigvecs, (0, 1, 3, 2, 4))
    s_view = jnp.transpose(solutions, (0, 1, 2, 3, 5, 4, 6))
    s_view = s_view.reshape(2, times, pairs, COLORS, SPINS, blocks, LANES)
    s_view = jnp.swapaxes(s_view, 4, 5).reshape(2, times, pairs, rows, LANES)
    s_view = pltpu.with_memory_space_constraint(s_view, pltpu.HBM)
    vmem = pl.BlockSpec(memory_space=pltpu.VMEM)
    params = pltpu.CompilerParams(vmem_limit_bytes=VMEM_BYTES)
    split, sums = pl.pallas_call(
        split_kernel,
        out_shape=(
            jax.ShapeDtypeStruct((times, COLORS * blocks, 4 * columns, LANES), BF16),
            jax.ShapeDtypeStruct((pairs, LANES), F32),
        ),
        in_specs=[pl.BlockSpec(memory_space=pltpu.HBM)],
        out_specs=(vmem, vmem),
        scratch_shapes=[
            pltpu.VMEM((2, times, pairs, pitch, LANES), F32),
            pltpu.SemaphoreType.DMA((2, times, COLORS)),
        ],
        compiler_params=params,
        name="split",
        cost_estimate=pl.CostEstimate(
            flops=solutions.size, bytes_accessed=8 * solutions.size, transcendentals=0
        ),
    )(s_view)
    norm_row = pl.pallas_call(
        functools.partial(row_kernel, columns=columns),
        out_shape=jax.ShapeDtypeStruct((8, LANES), F32),
        in_specs=[vmem],
        out_specs=vmem,
        compiler_params=params,
        name="row",
        cost_estimate=pl.CostEstimate(flops=10**9, bytes_accessed=10**7, transcendentals=0),
    )(sums)
    tiles = jax.ShapeDtypeStruct((eigs // 8, 2 * times, 8, LANES), F32)
    block = jax.ShapeDtypeStruct((2, 2, 2 * times, 8, LANES), F32)
    make_tiles = pl.pallas_call(
        functools.partial(tile_kernel, masks=masks),
        out_shape=(block, block) if masks else tiles,
        in_specs=[vmem] * 2,
        out_specs=(vmem, vmem) if masks else vmem,
        scratch_shapes=[pltpu.VMEM(tiles.shape, F32)] if masks else [],
        compiler_params=params,
        name="tiles",
        cost_estimate=pl.CostEstimate(
            flops=24 * times * eigs * columns * COLORS * sites,
            bytes_accessed=4 * (eigvecs.size + solutions.size),
            transcendentals=0,
        ),
    )
    products = make_tiles(split, e_view)
    return products, norm_row


def finish_kernel(kept_ref, came_ref, sign_ref, out_ref):
    _, times, width = out_ref.shape
    columns = width // 8
    pairs = columns // SPINS
    row = lax.broadcasted_iota(jnp.int32, (8, LANES), 0)
    lane = lax.broadcasted_iota(jnp.int32, (8, LANES), 1)
    column = jnp.bitwise_and(lane + LANES - (row * columns) % LANES, LANES - 1)
    source = jnp.where(column < columns, (column % SPINS) * pairs + column // SPINS, 0)
    for part in range(2):
        for t in range(times):
            index = part * times + t
            tile = (kept_ref[index] + came_ref[index]) * sign_ref[t : t + 1, :]
            tile = jnp.take_along_axis(tile, source, axis=1)
            for piece in range(width // LANES):
                first = piece * LANES // columns
                edge = (first + 1) * columns - piece * LANES
                out_ref[part, t : t + 1, piece * LANES : (piece + 1) * LANES] = jnp.where(
                    lane[:1] < edge, tile[first : first + 1], tile[first + 1 : first + 2]
                )


def norm_kernel(kept_ref, extra_ref, norm_ref, *, first, cells):
    src_count, col_count = norm_ref.shape
    total = kept_ref[...] + extra_ref[...]
    for src in range(src_count):
        shift = 2 * LANES - first - src * col_count
        norm = pltpu.roll(total, shift % LANES, 1)
        norm_ref[src : src + 1, :] = norm[:1, :col_count] / cells


def swap(x, ta_mask, sa_mask):
    ta_size, sa_size = lax.axis_size("ta"), lax.axis_size("sa")
    pairs = [
        (ta * sa_size + sa, (ta ^ ta_mask) * sa_size + (sa ^ sa_mask))
        for ta in range(ta_size)
        for sa in range(sa_size)
    ]
    return lax.ppermute(x, ("ta", "sa"), pairs)


def radices_of(count):
    found = []
    for prime in (2, 3, 5, 7, 11, 13):
        while count % prime == 0:
            found.append(prime)
            count //= prime
    return found + ([count] if count > 1 else [])


def shifted(size, weight, radix, shift):
    moves = []
    for source in range(size):
        own = (source // weight) % radix
        moves.append((source, source + ((own + shift) % radix - own) * weight))
    return moves


def scatter_sum(blocks, axis):
    size = lax.axis_size(axis)
    me = lax.axis_index(axis)
    radices = radices_of(size)
    held = blocks.reshape(tuple(reversed(radices)) + blocks.shape[1:])
    weight = 1
    for depth, radix in enumerate(radices):
        dim = len(radices) - 1 - depth
        digit = (me // weight) % radix
        total = lax.dynamic_index_in_dim(held, digit, dim, False)
        for shift in range(1, radix):
            send = lax.dynamic_index_in_dim(held, (digit + shift) % radix, dim, False)
            total = total + lax.ppermute(send, axis, shifted(size, weight, radix, shift))
        held = total
        weight *= radix
    return held


def all_sum(x, axis):
    size = lax.axis_size(axis)
    weight = 1
    for radix in radices_of(size):
        total = x
        for shift in range(1, radix):
            total = total + lax.ppermute(x, axis, shifted(size, weight, radix, shift))
        x = total
        weight *= radix
    return x


def on_device(eigvecs, solutions, source_times, spin_dilution):
    _, times, eigs, _, sites = eigvecs.shape
    src_count, col_count = spin_dilution.shape
    pairs = src_count * col_count
    columns = pairs * SPINS
    devices = lax.axis_size("sa")
    cells = 12.0 * times * lax.axis_size("ta") * sites * devices
    own_width = eigs * columns // devices

    crossed = devices == 8 and lax.axis_size("ta") == 4 and eigs == 64 and columns == 96
    tiles, norm_row = local_tiles(eigvecs, solutions, MASKS if crossed else None)
    slice_times = lax.axis_index("ta") * times + jnp.arange(times, dtype=jnp.int32)
    boundary = jnp.where(slice_times[:, None] < source_times[None, :], -1.0, 1.0).astype(F32)
    chirality = jnp.where(spin_dilution < 2, 1.0, -1.0).astype(F32)
    signs = (boundary[:, :, None] * chirality[None]).reshape(times, pairs)
    if crossed:
        first = lax.broadcasted_iota(jnp.int32, (2 * times, 1, 1), 0) == 0
        own = norm_row
        for ta_mask in (3, 1, 2):
            norm_row = norm_row + swap(own, ta_mask, 1)
        kept, sent = tiles
        held = kept + swap(sent, 0, MASKS[0]) + jnp.where(first, norm_row, 0.0)
        held = held[0] + swap(held[1], 0, MASKS[1])
        kept, came = held[0], swap(held[1], 0, MASKS[2])
        line = kept[0] + came[0]
        extra = swap(line, 0, 1)
        lanes = jnp.concatenate(
            [signs] * SPINS + [jnp.ones((times, LANES - columns), F32)], 1
        )
        vmem = pl.BlockSpec(memory_space=pltpu.VMEM)
        params = pltpu.CompilerParams(vmem_limit_bytes=VMEM_BYTES)
        values = pl.pallas_call(
            finish_kernel,
            out_shape=jax.ShapeDtypeStruct((2, times, own_width), F32),
            in_specs=[vmem] * 3,
            out_specs=vmem,
            compiler_params=params,
            name="finish",
            cost_estimate=pl.CostEstimate(flops=10**7, bytes_accessed=10**6, transcendentals=0),
        )(kept, came, lanes)
        norms = pl.pallas_call(
            functools.partial(norm_kernel, first=columns, cells=cells),
            out_shape=jax.ShapeDtypeStruct((src_count, col_count), F32),
            in_specs=[vmem] * 2,
            out_specs=vmem,
            compiler_params=params,
            name="norms",
        )(line, extra)
        return values, norms
    norm_row = lax.psum(norm_row[0, columns : columns + pairs], "sa")
    values = tiles.reshape(eigs // 8, 2, times, 8, LANES)[..., :columns]
    values = values.reshape(eigs // 8, 2, times, 8, SPINS, pairs)
    values = values * signs[None, None, :, None, None]
    values = jnp.transpose(values, (1, 2, 0, 3, 5, 4)).reshape(2, times, devices, own_width)
    values = scatter_sum(jnp.transpose(values, (2, 0, 1, 3)), "sa")
    norms = all_sum(norm_row.reshape(src_count, col_count), "ta") / cells
    return values, norms


def solution(mesh):
    return jax.shard_map(
        on_device,
        mesh=mesh,
        in_specs=(
            P(None, "ta", None, None, "sa"),
            P(None, "ta", None, None, None, None, "sa"),
            P(),
            P(),
        ),
        out_specs=(P(None, "ta", "sa"), P()),
        check_vma=False,
    )
```
